16 devices in a mesh: dp: 4 (over y, z, core), sp: 4 (over x).
Axes of the slice: x: 4, y: 2, z: 1, core: 2. Of those that a mesh axis runs over, the one named last changes fastest.
The devices are a block of a 4x4x8 slice.
Arguments:
- q: bfloat16 [128, 8, 256], P('dp'), parts along dimension 0
- k: bfloat16 [128, 2048, 8, 256], P('dp', 'sp'), parts along dimension 0
- v: bfloat16 [128, 2048, 8, 256], P('dp', 'sp'), parts along dimension 0
Outputs:
- q: bfloat16 [128, 8, 256], P('dp'), parts along dimension 0
There are 4 independent parts. The reference program is written for one: setup_inputs(seed, part) draws one part's arguments, and reference() takes and returns one part's arrays. A program takes and returns all parts, laid end to end along the dimension named above; each array names one.
All inputs are finite; a program needn't handle non-finite values.
Results may differ from the reference program's by a relative error of at most 0.012.
Values are sent between devices in bfloat16 or wider.
A program may use at most 768 MiB of HBM per device.

```python
import jax
import jax.numpy as jnp

BATCH = 32
CACHE = 2048
HEADS = 8
KV_HEADS = 8
HEAD = 256


def setup_inputs(seed: int = 0, part: int = 0) -> dict:
    kq, kk, kv = (jax.random.fold_in(k, part) for k in jax.random.split(jax.random.key(seed), 3))
    return {
        "q": (3 * jax.random.normal(kq, (BATCH, HEADS, HEAD), jnp.float32)).astype(jnp.bfloat16),
        "k": jax.random.normal(kk, (BATCH, CACHE, KV_HEADS, HEAD), jnp.float32).astype(jnp.bfloat16),
        "v": jax.random.normal(kv, (BATCH, CACHE, KV_HEADS, HEAD), jnp.float32).astype(jnp.bfloat16),
    }


def einsum(form, a, b):
    return jnp.einsum(form, a.astype(jnp.float32), b.astype(jnp.float32))


def reference(q, k, v):
    grouped = q.reshape(BATCH, KV_HEADS, -1, HEAD)
    scores = einsum("bgsd,bugd->bgsu", grouped, k) * HEAD**-0.5
    weights = jax.nn.softmax(scores, -1).astype(jnp.bfloat16)
    return einsum("bgsu,bugd->bgsd", weights, v).astype(jnp.bfloat16).reshape(BATCH, HEADS, HEAD)
```

```python
import functools

import jax
import jax.numpy as jnp
from jax import lax
from jax.experimental import pallas as pl
from jax.experimental.pallas import tpu as pltpu
from jax.sharding import PartitionSpec as P

SLOTS = 6


def kernel(axis, runs, scale, q_ref, k_ref, v_ref, out_ref, k_buf, v_buf, parts, k_sem, v_sem, send_sem, recv_sem):
    count, rows, head = k_ref.shape
    heads = q_ref.shape[1]
    me = lax.axis_index(axis)

    def fetch(b):
        slot = lax.rem(b, SLOTS)
        pltpu.make_async_copy(k_ref.at[b], k_buf.at[slot], k_sem.at[slot]).start()
        pltpu.make_async_copy(v_ref.at[b], v_buf.at[slot], v_sem.at[slot]).start()

    for b in range(SLOTS):
        fetch(b)

    barrier = pltpu.get_barrier_semaphore()
    for ahead in range(1, runs):
        pl.semaphore_signal(barrier, inc=1, device_id={axis: lax.rem(me + ahead, runs)})
    pl.semaphore_wait(barrier, runs - 1)

    own = lax.broadcasted_iota(jnp.int32, (heads, rows), 1) % heads == lax.broadcasted_iota(jnp.int32, (heads, rows), 0)

    def send(b, ahead):
        return pltpu.make_async_remote_copy(
            src_ref=parts.at[0, b],
            dst_ref=parts.at[ahead, b],
            send_sem=send_sem.at[ahead - 1, b],
            recv_sem=recv_sem.at[ahead - 1, b],
            device_id={axis: lax.rem(me + ahead, runs)},
        )

    def attend(b, _):
        slot = lax.rem(b, SLOTS)
        pltpu.make_async_copy(k_ref.at[b], k_buf.at[slot], k_sem.at[slot]).wait()
        scores = lax.dot_general(q_ref[b], k_buf[slot], (((1,), (1,)), ((), ())), preferred_element_type=jnp.float32)
        scores = jnp.where(own, scores * scale, -jnp.inf)
        high = jnp.max(scores, -1, keepdims=True)
        weights = jnp.exp(scores - high)
        total = jnp.sum(weights, -1, keepdims=True)
        pltpu.make_async_copy(v_ref.at[b], v_buf.at[slot], v_sem.at[slot]).wait()
        seen = jnp.dot(weights.astype(jnp.bfloat16), v_buf[slot], preferred_element_type=jnp.float32)
        parts[0, b, :, :head] = seen
        lane = lax.broadcasted_iota(jnp.int32, (heads, 128), 1)
        parts[0, b, :, head:] = jnp.where(lane < 64, total, high)
        for ahead in range(1, runs):
            send(b, ahead).start()

        @pl.when(b + SLOTS < count)
        def _():
            fetch(b + SLOTS)

        return 0

    lax.fori_loop(0, count, attend, 0)

    def finish(b, _):
        for ahead in range(1, runs):
            send(b, ahead).wait()
        total = [parts[run, b, :, head : head + 1] for run in range(runs)]
        high = [parts[run, b, :, head + 64 : head + 65] for run in range(runs)]
        top = functools.reduce(jnp.maximum, high)
        rescale = [jnp.exp(h - top) for h in high]
        seen = sum(parts[run, b, :, :head] * rescale[run] for run in range(runs))
        out_ref[b] = (seen / sum(t * r for t, r in zip(total, rescale))).astype(out_ref.dtype)
        return 0

    lax.fori_loop(0, count, finish, 0)


def solution(mesh):
    axis = "sp"
    runs = mesh.shape[axis]

    def step(q, k, v):
        count, tokens, heads, head = k.shape
        rows = tokens * heads
        return pl.pallas_call(
            functools.partial(kernel, axis, runs, head**-0.5),
            out_shape=jax.ShapeDtypeStruct(q.shape, q.dtype),
            in_specs=[
                pl.BlockSpec(memory_space=pltpu.VMEM),
                pl.BlockSpec(memory_space=pl.ANY),
                pl.BlockSpec(memory_space=pl.ANY),
            ],
            out_specs=pl.BlockSpec(memory_space=pltpu.VMEM),
            scratch_shapes=[
                pltpu.VMEM((SLOTS, rows, head), k.dtype),
                pltpu.VMEM((SLOTS, rows, head), v.dtype),
                pltpu.VMEM((runs, count, heads, head + 128), jnp.float32),
                pltpu.SemaphoreType.DMA((SLOTS,)),
                pltpu.SemaphoreType.DMA((SLOTS,)),
                pltpu.SemaphoreType.DMA((runs - 1, count)),
                pltpu.SemaphoreType.DMA((runs - 1, count)),
            ],
            compiler_params=pltpu.CompilerParams(
                collective_id=0, has_side_effects=True, vmem_limit_bytes=56 << 20
            ),
            name="attend",
        )(q, k.reshape(count, rows, head), v.reshape(count, rows, head))

    return jax.shard_map(
        step,
        mesh=mesh,
        in_specs=(P("dp", None, None), P("dp", "sp", None, None), P("dp", "sp", None, None)),
        out_specs=P("dp", None, None),
        check_vma=False,
    )
```

```python
import functools

import jax
import jax.numpy as jnp
from jax import lax
from jax.experimental import pallas as pl
from jax.experimental.pallas import tpu as pltpu
from jax.sharding import PartitionSpec as P

PAIR = 2
SLOTS = 4
PIECES = 4
UNROLL = 5
LEAD = 2
LANES = 128


def kernel(axis, runs, scale, q_hbm, k_ref, v_ref, out_ref, q_ref, k_buf, v_buf, even, odd, seen, stats, q_sem, k_sem, v_sem, last_sem, send_sem, recv_sem):
    _, heads, head = q_ref.shape
    count, rows, _ = k_ref.shape
    steps = count // PAIR
    me = lax.axis_index(axis)

    def k_copy(i):
        slot = lax.rem(i, SLOTS)
        return pltpu.make_async_copy(k_ref.at[pl.ds(i * PAIR, PAIR)], k_buf.at[slot], k_sem.at[slot])

    def v_copy(i):
        slot = lax.rem(i, SLOTS)
        return pltpu.make_async_copy(v_ref.at[pl.ds(i * PAIR, PAIR)], v_buf.at[slot], v_sem.at[slot])

    pieces = ((0, 0, rows), (1, 0, rows // 2), (1, rows // 2, rows // 4), (1, 3 * rows // 4, rows // 4))
    last_slot = (steps - 1) % SLOTS

    def last_copy(piece):
        j, start, size = pieces[piece]
        part = pl.ds(start, size)
        return pltpu.make_async_copy(
            v_ref.at[count - PAIR + j, part], v_buf.at[last_slot, j, part], last_sem.at[piece]
        )

    q_copy = pltpu.make_async_copy(q_hbm, q_ref, q_sem)
    q_copy.start()
    for i in range(SLOTS):
        k_copy(i).start()
    for i in range(SLOTS):
        v_copy(i).start()

    barrier = pltpu.get_barrier_semaphore()
    for ahead in range(1, runs):
        pl.semaphore_signal(barrier, inc=1, device_id={axis: lax.rem(me + ahead, runs)})

    lane = lax.broadcasted_iota(jnp.int32, (heads, LANES), 1)
    own = lane % heads == lax.broadcasted_iota(jnp.int32, (heads, LANES), 0)
    quarter = lane // (LANES // 4)

    EARLY_SEEN, EARLY_STATS, LAST_SEEN, LAST_STATS = range(4)

    def to_peers(kind, index):
        ref = seen if kind in (EARLY_SEEN, LAST_SEEN) else stats
        for ahead in range(1, runs):
            yield pltpu.make_async_remote_copy(
                src_ref=ref.at[me, index],
                dst_ref=ref.at[me, index],
                send_sem=send_sem.at[kind % 2, ahead - 1],
                recv_sem=recv_sem.at[kind, ahead - 1],
                device_id={axis: lax.rem(me + ahead, runs)},
            )

    def send(kind, index):
        for copy in to_peers(kind, index):
            copy.start()

    def received(kind, index):
        for copy in to_peers(kind, index):
            copy.wait_recv()

    def score(i, scores, tops):
        slot = lax.rem(i, SLOTS)
        for j in range(PAIR):
            s = lax.dot_general(
                q_ref[i * PAIR + j], k_buf[slot, j], (((1,), (1,)), ((), ())), preferred_element_type=jnp.float32
            )
            s = [jnp.where(own, s[:, c : c + LANES] * scale, -jnp.inf) for c in range(0, rows, LANES)]
            high = jnp.max(functools.reduce(jnp.maximum, s), -1, keepdims=True)
            tops[j] = jnp.broadcast_to(high, (heads, LANES))
            scores[j] = jnp.concatenate(s, 1)

    def weigh(scores, tops, weights, totals):
        for j in range(PAIR):
            high = tops[j]
            total = None
            for c in range(0, rows, LANES):
                w = jnp.exp(scores[j, :, c : c + LANES] - high)
                total = w if total is None else total + w
                weights[j, :, c : c + LANES] = w.astype(weights.dtype)
            totals[j] = jnp.broadcast_to(jnp.sum(total, -1, keepdims=True), (heads, LANES))

    def mix(weights, slot, j, start, size):
        part = pl.ds(start, size)
        return jnp.dot(weights[j, :, part], v_buf[slot, j, part], preferred_element_type=jnp.float32)

    def gathered(totals, tops):
        return jnp.where(
            quarter == 0, totals[0], jnp.where(quarter == 1, tops[0], jnp.where(quarter == 2, totals[1], tops[1]))
        )

    def combine(i):
        stat = [stats[run, i] for run in range(runs)]
        wide = LANES // 4
        for j in range(PAIR):
            total = [s[:, 2 * wide * j : 2 * wide * j + 1] for s in stat]
            high = [s[:, 2 * wide * j + wide : 2 * wide * j + wide + 1] for s in stat]
            top = functools.reduce(jnp.maximum, high)
            rescale = [jnp.exp(h - top) for h in high]
            over = 1 / sum(t * r for t, r in zip(total, rescale))
            b = i * PAIR + j
            out_ref[b] = sum(seen[run, b].astype(jnp.float32) * (r * over) for run, r in enumerate(rescale)).astype(
                out_ref.dtype
            )

    q_copy.wait()

    for i in range(LEAD):
        k_copy(i).wait()
        score(i, *(even, odd)[i % 2][:2])
        k_copy(i + SLOTS).start()
    weigh(*even)
    pl.semaphore_wait(barrier, runs - 1)

    def advance(i, this, other, more):
        if more:
            k_copy(i + LEAD).wait()
        v_copy(i).wait()
        _, tops, weights, totals = this
        own_totals, own_tops = totals[...], tops[...]
        if more:
            score(i + LEAD, *this[:2])
        weigh(*other)
        for j in range(PAIR):
            seen[me, i * PAIR + j] = mix(weights, lax.rem(i, SLOTS), j, 0, rows).astype(seen.dtype)
        stats[me, i] = gathered(own_totals, own_tops)
        send(EARLY_SEEN, pl.ds(i * PAIR, PAIR))
        send(EARLY_STATS, i)

    def refill(i):
        @pl.when(i + LEAD + SLOTS < steps)
        def _():
            k_copy(i + LEAD + SLOTS).start()

        @pl.when(i + SLOTS < steps - 1)
        def _():
            v_copy(i + SLOTS).start()

        @pl.when(i + SLOTS == steps - 1)
        def _():
            for piece in range(PIECES):
                last_copy(piece).start()

    def body(m, _):
        advance(2 * m, even, odd, True)
        refill(2 * m)
        advance(2 * m + 1, odd, even, True)
        refill(2 * m + 1)
        return 0

    lax.fori_loop(0, (steps - LEAD) // 2, body, 0)
    advance(steps - 2, even, odd, False)
    _, tops, weights, totals = odd
    stats[me, steps - 1] = gathered(totals[...], tops[...])
    send(LAST_STATS, steps - 1)
    sums = None
    for piece, (j, start, size) in enumerate(pieces):
        last_copy(piece).wait()
        more = mix(weights, last_slot, j, start, size)
        sums = more if start == 0 else sums + more
        if start + size == rows:
            seen[me, count - PAIR + j] = sums.astype(seen.dtype)
            send(LAST_SEEN, count - PAIR + j)

    received(EARLY_SEEN, pl.ds(0, count - PAIR))
    received(EARLY_STATS, pl.ds(0, steps - 1))

    def finish(i, _):
        combine(i)
        return 0

    lax.fori_loop(0, steps - 1, finish, 0, unroll=UNROLL)
    received(LAST_STATS, steps - 1)
    received(LAST_SEEN, pl.ds(count - PAIR, PAIR))
    combine(steps - 1)
    for kind, index in ((EARLY_SEEN, pl.ds(0, count)), (EARLY_STATS, pl.ds(0, steps))):
        for copy in to_peers(kind, index):
            copy.wait_send()


def solution(mesh):
    axis = "sp"
    runs = mesh.shape[axis]

    def step(q, k, v):
        count, tokens, heads, head = k.shape
        rows = tokens * heads
        steps = count // PAIR
        step_buffers = (
            pltpu.VMEM((PAIR, heads, rows), jnp.float32),
            pltpu.VMEM((PAIR, heads, LANES), jnp.float32),
            pltpu.VMEM((PAIR, heads, rows), v.dtype),
            pltpu.VMEM((PAIR, heads, LANES), jnp.float32),
        )
        return pl.pallas_call(
            functools.partial(kernel, axis, runs, head**-0.5),
            out_shape=jax.ShapeDtypeStruct(q.shape, q.dtype),
            in_specs=[pl.BlockSpec(memory_space=pltpu.HBM)] * 3,
            out_specs=pl.BlockSpec(memory_space=pltpu.VMEM),
            scratch_shapes=[
                pltpu.VMEM(q.shape, q.dtype),
                pltpu.VMEM((SLOTS, PAIR, rows, head), k.dtype),
                pltpu.VMEM((SLOTS, PAIR, rows, head), v.dtype),
                step_buffers,
                step_buffers,
                pltpu.VMEM((runs, count, heads, head), q.dtype),
                pltpu.VMEM((runs, steps, heads, LANES), jnp.float32),
                pltpu.SemaphoreType.DMA,
                pltpu.SemaphoreType.DMA((SLOTS,)),
                pltpu.SemaphoreType.DMA((SLOTS,)),
                pltpu.SemaphoreType.DMA((PIECES,)),
                pltpu.SemaphoreType.DMA((2, runs - 1)),
                pltpu.SemaphoreType.DMA((4, runs - 1)),
            ],
            compiler_params=pltpu.CompilerParams(
                collective_id=0, has_side_effects=True, vmem_limit_bytes=40 << 20
            ),
            name="attend",
        )(pltpu.with_memory_space_constraint(q, pltpu.HBM), k.reshape(count, rows, head), v.reshape(count, rows, head))

    return jax.shard_map(
        step,
        mesh=mesh,
        in_specs=(P("dp", None, None), P("dp", "sp", None, None), P("dp", "sp", None, None)),
        out_specs=P("dp", None, None),
        check_vma=False,
    )
```

```python
import functools

import jax
import jax.numpy as jnp
from jax import lax
from jax.experimental import pallas as pl
from jax.experimental.pallas import tpu as pltpu
from jax.sharding import PartitionSpec as P

PAIR = 2
SLOTS = 4
PIECES = 2
UNROLL = 5
LEAD = 3
LANES = 128


def kernel(axis, runs, scale, q_hbm, k_ref, v_ref, out_ref, q_ref, k_buf, v_buf, sets, seen, stats, q_sem, k_sem, v_sem, last_sem, send_sem, recv_sem):
    _, heads, head = q_ref.shape
    count, rows, _ = k_ref.shape
    steps = count // PAIR
    me = lax.axis_index(axis)

    def k_copy(i):
        slot = lax.rem(i, SLOTS)
        return pltpu.make_async_copy(k_ref.at[pl.ds(i * PAIR, PAIR)], k_buf.at[slot], k_sem.at[slot])

    def v_copy(i):
        slot = lax.rem(i, SLOTS)
        return pltpu.make_async_copy(v_ref.at[pl.ds(i * PAIR, PAIR)], v_buf.at[slot], v_sem.at[slot])

    pieces = [(0, 3 * rows // 4), (3 * rows // 4, rows // 4)]
    last_slot = (steps - 1) % SLOTS

    def last_copy(piece):
        part = pl.ds(*pieces[piece])
        return pltpu.make_async_copy(
            v_ref.at[pl.ds(count - PAIR, PAIR), part], v_buf.at[last_slot, :, part], last_sem.at[piece]
        )

    q_copy = pltpu.make_async_copy(q_hbm, q_ref, q_sem)
    q_copy.start()
    for i in range(SLOTS):
        k_copy(i).start()
    for i in range(SLOTS - LEAD):
        v_copy(i).start()

    barrier = pltpu.get_barrier_semaphore()
    for ahead in range(1, runs):
        pl.semaphore_signal(barrier, inc=1, device_id={axis: lax.rem(me + ahead, runs)})

    lane = lax.broadcasted_iota(jnp.int32, (heads, LANES), 1)
    own = lane % heads == lax.broadcasted_iota(jnp.int32, (heads, LANES), 0)
    quarter = lane // (LANES // 4)

    EARLY_SEEN, EARLY_STATS, LAST_SEEN, LAST_STATS = range(4)

    def to_peers(kind, index):
        ref = seen if kind in (EARLY_SEEN, LAST_SEEN) else stats
        for ahead in range(1, runs):
            yield pltpu.make_async_remote_copy(
                src_ref=ref.at[me, index],
                dst_ref=ref.at[me, index],
                send_sem=send_sem.at[kind % 2, ahead - 1],
                recv_sem=recv_sem.at[kind, ahead - 1],
                device_id={axis: lax.rem(me + ahead, runs)},
            )

    def send(kind, index):
        for copy in to_peers(kind, index):
            copy.start()

    def received(kind, index):
        for copy in to_peers(kind, index):
            copy.wait_recv()

    def score(i, scores, tops):
        slot = lax.rem(i, SLOTS)
        for j in range(PAIR):
            s = lax.dot_general(
                q_ref[i * PAIR + j], k_buf[slot, j], (((1,), (1,)), ((), ())), preferred_element_type=jnp.float32
            )
            s = [jnp.where(own, s[:, c : c + LANES] * scale, -jnp.inf) for c in range(0, rows, LANES)]
            high = jnp.max(functools.reduce(jnp.maximum, s), -1, keepdims=True)
            tops[j] = jnp.broadcast_to(high, (heads, LANES))
            scores[j] = jnp.concatenate(s, 1)

    def weigh(scores, tops, weights, totals):
        for j in range(PAIR):
            high = tops[j]
            total = None
            for c in range(0, rows, LANES):
                w = jnp.exp(scores[j, :, c : c + LANES] - high)
                total = w if total is None else total + w
                weights[j, :, c : c + LANES] = w.astype(weights.dtype)
            totals[j] = jnp.broadcast_to(jnp.sum(total, -1, keepdims=True), (heads, LANES))

    def mix(weights, slot, j, start, size):
        part = pl.ds(start, size)
        return jnp.dot(weights[j, :, part], v_buf[slot, j, part], preferred_element_type=jnp.float32)

    def gathered(totals, tops):
        return jnp.where(
            quarter == 0, totals[0], jnp.where(quarter == 1, tops[0], jnp.where(quarter == 2, totals[1], tops[1]))
        )

    def combine(i):
        stat = [stats[run, i] for run in range(runs)]
        wide = LANES // 4
        for j in range(PAIR):
            total = [s[:, 2 * wide * j : 2 * wide * j + 1] for s in stat]
            high = [s[:, 2 * wide * j + wide : 2 * wide * j + wide + 1] for s in stat]
            top = functools.reduce(jnp.maximum, high)
            rescale = [jnp.exp(h - top) for h in high]
            over = 1 / sum(t * r for t, r in zip(total, rescale))
            b = i * PAIR + j
            out_ref[b] = sum(seen[run, b].astype(jnp.float32) * (r * over) for run, r in enumerate(rescale)).astype(
                out_ref.dtype
            )

    q_copy.wait()

    for i in range(LEAD):
        k_copy(i).wait()
        score(i, *sets[i][:2])
        k_copy(i + SLOTS).start()
        v_copy(i + SLOTS - LEAD).start()
    weigh(*sets[0])
    pl.semaphore_wait(barrier, runs - 1)

    def advance(i, turn, more):
        this, other = sets[turn], sets[(turn + 1) % LEAD]
        if more:
            k_copy(i + LEAD).wait()
        v_copy(i).wait()
        _, tops, weights, totals = this
        own_totals, own_tops = totals[...], tops[...]
        if more:
            score(i + LEAD, *this[:2])
        weigh(*other)
        for j in range(PAIR):
            seen[me, i * PAIR + j] = mix(weights, lax.rem(i, SLOTS), j, 0, rows).astype(seen.dtype)
        stats[me, i] = gathered(own_totals, own_tops)
        send(EARLY_SEEN, pl.ds(i * PAIR, PAIR))
        send(EARLY_STATS, i)

    def refill(i):
        @pl.when(i + LEAD + SLOTS < steps)
        def _():
            k_copy(i + LEAD + SLOTS).start()

        @pl.when(i + SLOTS < steps - 1)
        def _():
            v_copy(i + SLOTS).start()

        @pl.when(i + SLOTS == steps - 1)
        def _():
            for piece in range(PIECES):
                last_copy(piece).start()

    def body(m, _):
        for turn in range(LEAD):
            advance(LEAD * m + turn, turn, True)
            refill(LEAD * m + turn)
        return 0

    looped = (steps - LEAD) // LEAD
    lax.fori_loop(0, looped, body, 0)
    for i in range(LEAD * looped, steps - 1):
        advance(i, i % LEAD, i + LEAD < steps)
    _, tops, weights, totals = sets[(steps - 1) % LEAD]
    stats[me, steps - 1] = gathered(totals[...], tops[...])
    send(LAST_STATS, steps - 1)
    sums = [0.0] * PAIR
    for piece, (start, size) in enumerate(pieces):
        last_copy(piece).wait()
        sums = [sums[j] + mix(weights, last_slot, j, start, size) for j in range(PAIR)]
    for j in range(PAIR):
        seen[me, count - PAIR + j] = sums[j].astype(seen.dtype)
    send(LAST_SEEN, pl.ds(count - PAIR, PAIR))

    received(EARLY_SEEN, pl.ds(0, count - PAIR))
    received(EARLY_STATS, pl.ds(0, steps - 1))

    def finish(i, _):
        combine(i)
        return 0

    lax.fori_loop(0, steps - 1, finish, 0, unroll=UNROLL)
    received(LAST_STATS, steps - 1)
    received(LAST_SEEN, pl.ds(count - PAIR, PAIR))
    combine(steps - 1)
    for kind, index in ((EARLY_SEEN, pl.ds(0, count)), (EARLY_STATS, pl.ds(0, steps))):
        for copy in to_peers(kind, index):
            copy.wait_send()


def solution(mesh):
    axis = "sp"
    runs = mesh.shape[axis]

    def step(q, k, v):
        count, tokens, heads, head = k.shape
        rows = tokens * heads
        steps = count // PAIR
        step_buffers = (
            pltpu.VMEM((PAIR, heads, rows), jnp.float32),
            pltpu.VMEM((PAIR, heads, LANES), jnp.float32),
            pltpu.VMEM((PAIR, heads, rows), v.dtype),
            pltpu.VMEM((PAIR, heads, LANES), jnp.float32),
        )
        return pl.pallas_call(
            functools.partial(kernel, axis, runs, head**-0.5),
            out_shape=jax.ShapeDtypeStruct(q.shape, q.dtype),
            in_specs=[pl.BlockSpec(memory_space=pltpu.HBM)] * 3,
            out_specs=pl.BlockSpec(memory_space=pltpu.VMEM),
            scratch_shapes=[
                pltpu.VMEM(q.shape, q.dtype),
                pltpu.VMEM((SLOTS, PAIR, rows, head), k.dtype),
                pltpu.VMEM((SLOTS, PAIR, rows, head), v.dtype),
                (step_buffers,) * LEAD,
                pltpu.VMEM((runs, count, heads, head), q.dtype),
                pltpu.VMEM((runs, steps, heads, LANES), jnp.float32),
                pltpu.SemaphoreType.DMA,
                pltpu.SemaphoreType.DMA((SLOTS,)),
                pltpu.SemaphoreType.DMA((SLOTS,)),
                pltpu.SemaphoreType.DMA((PIECES,)),
                pltpu.SemaphoreType.DMA((2, runs - 1)),
                pltpu.SemaphoreType.DMA((4, runs - 1)),
            ],
            compiler_params=pltpu.CompilerParams(
                collective_id=0, has_side_effects=True, vmem_limit_bytes=40 << 20
            ),
            name="attend",
        )(pltpu.with_memory_space_constraint(q, pltpu.HBM), k.reshape(count, rows, head), v.reshape(count, rows, head))

    return jax.shard_map(
        step,
        mesh=mesh,
        in_specs=(P("dp", None, None), P("dp", "sp", None, None), P("dp", "sp", None, None)),
        out_specs=P("dp", None, None),
        check_vma=False,
    )
```
